128 devices in a mesh: row: 16 (over y, x), col: 8 (over z, core).
Axes of the slice: x: 4, y: 4, z: 4, core: 2. Of those that a mesh axis runs over, the one named last changes fastest.
Arguments:
- a_window: float32 [16384, 8192], P('row', 'col'), may hold values from -6 to 6
- l_panel: float32 [16384, 1024], P('row'), may hold values from -0.1875 to 0.1875
- l_inverse: float32 [2, 512, 512], replicated, may hold values from -2 to 2, as said below
Outputs:
- reduced: float32 [16384, 8192], P('row', 'col')
The draws below stay inside these ranges and needn't reach their ends.
Inputs may be any that keep to these rules, and one draw needn't show every extreme that they name: `l_inverse`: both blocks are lower triangular, with diagonal entries between 0.5 and 2.
All inputs are finite; a program needn't handle non-finite values.
Results may differ from the reference program's by a relative error of at most 0.000067.
Values sent between devices are 32-bit elements; how exact they have to be, the bound alone decides.
No kernel may reach another device: no remote copies, remote signals or barrier semaphores. Data moves between devices by JAX's collectives and lax.ppermute only.
A program may use at most 128 MiB of HBM per device.

```python
import jax
import jax.numpy as jnp
from jax import lax

N = 16384
B = 512
WC = 8192


def draw_l_inverse(key, part):
    first_key, second_key = jax.random.split(jax.random.fold_in(key, 17))
    spread = jnp.clip(jax.random.normal(first_key, (2, B, B), jnp.float32), -4.0, 4.0)
    diagonal = jax.random.uniform(second_key, (2, B), jnp.float32, 0.5, 1.5)
    strict = jnp.tril(spread, -1) / jnp.sqrt(jnp.float32(B))
    return strict + diagonal[:, :, None] * jnp.eye(B, dtype=jnp.float32)[None, :, :]


def shard_levels(own_key, extent, pieces, least, top_value):
    level, own = 1.0, jax.random.fold_in(own_key, 6)
    for axis_at, shards_of in pieces:
        steps = jnp.exp(jax.random.uniform(jax.random.fold_in(own, axis_at), (shards_of,), jnp.float32, least / len(pieces), top_value / len(pieces)))
        level = level * jnp.repeat(steps, extent[axis_at] // shards_of).reshape([-1 if axis == axis_at else 1 for axis in range(len(extent))])
    return level


def noise(own_key, shape, deviation, reach, cuts=(), kind=jnp.bfloat16):
    loudness = shard_levels(own_key, shape, cuts, -0.22, 0.18) if cuts else 1.0
    drawn = jax.random.normal(own_key, shape, jnp.float32) * deviation * loudness
    return jnp.minimum(jnp.maximum(drawn, -reach), reach).astype(kind)


def setup_inputs(seed: int = 0) -> dict:
    key_list = jax.random.split(jax.random.key(seed), 4)
    a_window = noise(key_list[0], (N, WC), 1.0, 6.0, ((0, 16), (1, 8)), jnp.float32)
    l_panel = noise(key_list[1], (N, 2 * B), (2 * B) ** -0.5, 0.1875, ((0, 16),), jnp.float32)
    l_inverse = draw_l_inverse(jax.random.fold_in(key_list[3], 71), 0)
    return {"a_window": a_window, "l_panel": l_panel, "l_inverse": l_inverse}


def matmul_hp(left, right):
    return jnp.dot(left, right, precision=lax.Precision.HIGHEST, preferred_element_type=jnp.float32)


def reference(a_window, l_panel, l_inverse):
    first_inv = l_inverse[0]
    second_inv = l_inverse[1]
    coupling = l_panel[B:2 * B, :B]
    leading = matmul_hp(a_window[:, :B], first_inv.T)
    second_col = matmul_hp(a_window[:, B:2 * B] - matmul_hp(leading, coupling.T), second_inv.T)
    solved = jnp.concatenate([leading, second_col], 1)
    upper_tile = matmul_hp(first_inv, solved[:B])
    lower_tile = matmul_hp(second_inv, solved[B:2 * B] - matmul_hp(coupling, upper_tile))
    diag_block = jnp.concatenate([upper_tile, lower_tile], 0)
    below = l_panel[2 * B:]
    product = matmul_hp(below, diag_block)
    reduced_g = solved[2 * B:] - 0.5 * product
    lower_panel = solved[2 * B:] - product
    width_left = WC - 2 * B
    update = a_window[2 * B:, 2 * B:] - matmul_hp(below, reduced_g[:width_left].T) - matmul_hp(reduced_g, below[:width_left].T)
    upper_rows = jnp.concatenate([diag_block, a_window[:2 * B, 2 * B:]], 1)
    lower_rows = jnp.concatenate([lower_panel, update], 1)
    return jnp.concatenate([upper_rows, lower_rows], 0)
```

```python
import jax
import jax.numpy as jnp
from jax import lax
from jax.sharding import PartitionSpec as P


BOTH = ("row", "col")
ROWS, COLS = 16, 8
HALF = 512
WIDE = 1024
CHUNK = WIDE // ROWS
PIECE = WIDE // COLS


def at(row, col):
    return row * COLS + col


def mm(left, right, left_dim=1, right_dim=0):
    return lax.dot_general(
        left,
        right,
        (((left_dim,), (right_dim,)), ((), ())),
        precision=lax.Precision.HIGH,
        preferred_element_type=jnp.float32,
    )


def move(value, pairs):
    return lax.ppermute(value, BOTH, pairs)


def to_chunks(block, row_at):
    got = [
        move(
            block(part),
            [(at(r, q), at(2 * q + part, r)) for r in range(COLS) for q in range(COLS)],
        )
        for part in range(2)
    ]
    return jnp.where(row_at % 2 == 0, got[0], got[1])


def body(a_window, l_panel, l_inverse):
    row_at = lax.axis_index("row")
    col_at = lax.axis_index("col")
    z_at, core = col_at // 2, col_at % 2
    inv0, inv1 = l_inverse[0], l_inverse[1]
    panel_col = col_at == 0

    own_l = to_chunks(
        lambda part: lax.dynamic_slice_in_dim(l_panel, PIECE * col_at + CHUNK * part, CHUNK, 0),
        row_at,
    )
    l_cols = lax.all_gather(own_l, "row", axis=0, tiled=True)

    flipped = a_window.T
    panel_t = jnp.where(row_at == 0, 0.5 * (a_window + flipped), flipped)
    piece = panel_t[:PIECE]
    for q in range(1, COLS):
        got = move(
            panel_t[PIECE * q : PIECE * (q + 1)], [(at(r, 0), at(r, q)) for r in range(ROWS)]
        )
        piece = jnp.where(col_at == q, got, piece)

    low = -mm(mm(inv1, l_panel[HALF:WIDE, :HALF]), inv0)
    low_part = lax.dynamic_slice_in_dim(low, 256 * core, 256, 0)
    for k in range(1, 4):
        got = move(low_part, [(at(0, c), at(4 * k, c)) for c in range(COLS)])
        low_part = jnp.where(row_at == 4 * k, got, low_part)
    for k in range(1, 4):
        got = move(low_part, [(at(4 * y, c), at(4 * y + k, c)) for y in range(4) for c in range(COLS)])
        low_part = jnp.where(row_at % 4 == k, got, low_part)
    other = move(low_part, [(at(r, c), at(r, c ^ 1)) for r in range(ROWS) for c in range(COLS)])
    low_all = jnp.where(
        core == 0,
        jnp.concatenate([low_part, other], 0),
        jnp.concatenate([other, low_part], 0),
    )

    first = mm(a_window[:, :HALF], inv0, 1, 1)
    second = mm(a_window[:, :HALF], low, 1, 1) + mm(a_window[:, HALF:], inv1, 1, 1)
    x_top = jnp.concatenate([first, second], 1)
    diag = jnp.concatenate(
        [mm(inv0, x_top[:HALF]), mm(low, x_top[:HALF]) + mm(inv1, x_top[HALF:])], 0
    )
    quarter = diag[:256]
    for k in range(1, 4):
        got = move(diag[256 * k : 256 * k + 256], [(at(0, 0), at(4 * k, 0))])
        quarter = jnp.where(row_at == 4 * k, got, quarter)
    h_chunk = quarter[:CHUNK]
    for k in range(1, 4):
        got = move(quarter[CHUNK * k : CHUNK * k + CHUNK], [(at(4 * y, 0), at(4 * y + k, 0)) for y in range(4)])
        h_chunk = jnp.where(row_at % 4 == k, got, h_chunk)

    d_first = mm(piece[:, :HALF], inv0, 1, 1)
    d_second = mm(piece[:, :HALF], low, 1, 1) + mm(piece[:, HALF:], inv1, 1, 1)
    ready = jnp.where(row_at == 0, jnp.concatenate([d_first, d_second], 1), piece)
    a_chunk = to_chunks(lambda part: ready[CHUNK * part : CHUNK * part + CHUNK], row_at)
    d_chunk = a_chunk
    got = move(d_chunk, [(at(r, 0), at(r, 4)) for r in range(ROWS)])
    d_chunk = jnp.where(col_at == 4, got, d_chunk)
    got = move(d_chunk, [(at(r, c), at(r, c + 2)) for r in range(ROWS) for c in (0, 4)])
    d_chunk = jnp.where(col_at % 4 == 2, got, d_chunk)
    got = move(d_chunk, [(at(r, c), at(r, c + 1)) for r in range(ROWS) for c in (0, 2, 4, 6)])
    d_chunk = jnp.where(core == 1, got, d_chunk)

    def z_pairs(flip):
        return [
            (at(r, 2 * z + c), at(r, 2 * (z ^ flip) + c))
            for r in range(ROWS)
            for z in range(4)
            for c in range(2)
        ]

    def z_gather(own, first_flip, second_flip):
        near = move(own, z_pairs(first_flip))
        far = move(jnp.stack([own, near]), z_pairs(second_flip))
        return {0: own, first_flip: near, second_flip: far[0], first_flip ^ second_flip: far[1]}

    sub0 = z_gather(piece[:CHUNK], 1, 3)
    sub1 = z_gather(piece[CHUNK:], 3, 1)
    mine = jnp.zeros((4, 2, CHUNK, WIDE), jnp.float32)
    for flip in range(4):
        both = jnp.stack([sub0[flip], sub1[flip]])[None]
        mine = lax.dynamic_update_slice_in_dim(mine, both, z_at ^ flip, 0)
    theirs = move(mine, [(at(r, c), at(r, c ^ 1)) for r in range(ROWS) for c in range(COLS)])
    row_t = jnp.where(
        core == 0, jnp.stack([mine, theirs], 1), jnp.stack([theirs, mine], 1)
    ).reshape(WIDE, WIDE)

    part = jnp.where(panel_col, h_chunk, a_chunk - mm(d_chunk, l_cols, 1, 1))
    gathered = lax.all_gather(part, "row", axis=0, tiled=True)

    y_rows = jnp.concatenate(
        [
            mm(l_panel[:, :HALF], inv0) + mm(l_panel[:, HALF:], low_all),
            mm(l_panel[:, HALF:], inv1),
        ],
        1,
    )
    x_rows = jnp.concatenate(
        [
            mm(row_t[:HALF], inv0, 0, 1),
            mm(row_t[:HALF], low_all, 0, 1) + mm(row_t[HALF:], inv1, 0, 1),
        ],
        1,
    )
    base = jnp.where(panel_col, x_rows, a_window - mm(x_rows, l_cols, 1, 1))
    left = jnp.where(panel_col, l_panel, y_rows)
    out = base - mm(left, gathered)
    top = jnp.where(panel_col, gathered, a_window)
    return jnp.where(row_at == 0, top, out)


def solution(mesh):
    placed = (P("row", "col"), P("row", None), P())
    return jax.shard_map(
        body, mesh=mesh, in_specs=placed, out_specs=P("row", "col"), check_vma=False
    )
```
